32 devices in a mesh: prob: 4 (over z), beam: 8 (over y, x, core).
Axes of the slice: x: 2, y: 2, z: 4, core: 2. Of those that a mesh axis runs over, the one named last changes fastest.
Arguments:
- queries: bfloat16 [512, 4096], P(('prob', 'beam')), parts along dimension 0, may hold values from -700 to 700
- new_keys: bfloat16 [512, 1024], P(('prob', 'beam')), parts along dimension 0, may hold values from -18 to 18
- new_values: bfloat16 [512, 1024], P(('prob', 'beam')), parts along dimension 0, may hold values from -12 to 12
- parents: int32 [512], P(('prob', 'beam')), parts along dimension 0, may hold values from 0 to 15, as said below
- page_counts: int32 [64], P(('prob', 'beam')), parts along dimension 0, may hold values from 1 to 4
- suffix_keys: bfloat16 [64, 512, 1024], P(('prob', 'beam')), parts along dimension 0, may hold values from -127 to 127, as said below
- suffix_values: bfloat16 [64, 512, 1024], P(('prob', 'beam')), parts along dimension 0, may hold values from -127 to 127, as said below
- suffix_scales: bfloat16 [64, 4, 2, 8], P(('prob', 'beam')), parts along dimension 0, may hold values from 0.024902344 to 0.044921875
- prefix_keys: bfloat16 [4096, 1024], P(('prob', 'beam')), parts along dimension 0, may hold values from -127 to 127, as said below
- prefix_values: bfloat16 [4096, 1024], P(('prob', 'beam')), parts along dimension 0, may hold values from -127 to 127, as said below
- prefix_scales: bfloat16 [32, 2, 8], P(('prob', 'beam')), parts along dimension 0, may hold values from 0.011962891 to 0.029907227
Outputs:
- attended: bfloat16 [512, 4096], P(('prob', 'beam')), parts along dimension 0
The draws below stay inside these ranges and needn't reach their ends.
There are 4 independent parts, one for each index of `prob`. The reference program is written for one: setup_inputs(seed, part) draws one part's arguments, and reference() takes and returns one part's arrays. A program takes and returns all parts, laid end to end along the dimension named above; each array names one. Nothing has to cross between parts.
Inputs may be any that keep to these rules, and one draw needn't show every extreme that they name: Device i of beam holds beams i * 2 to i * 2 + 1. Among the 16 children of one device at most 4 have parents held by one device. `suffix_keys`: whole numbers. `suffix_values`: whole numbers. `prefix_keys`: whole numbers. `prefix_values`: whole numbers.
All inputs are finite; a program needn't handle non-finite values.
Results may differ from the reference program's by a relative error of at most 0.0023.
Values may be sent and summed in bfloat16 or wider, within the bound.
No kernel may reach another device: no remote copies, remote signals or barrier semaphores. Data moves between devices by JAX's collectives and lax.ppermute only.
A program may use at most 128 MiB of HBM per device.

```python
import math
import jax
import jax.numpy as jnp
from jax import lax

HEADS = 32
KV_HEADS = 8
HEAD_DIM = 128
PAGE = 128
PAGES = 4
BEAM_DEV = 2
CHILD_DEV = 16
BEAMS = 16
CHILDREN = 128
PREFIX = 1024
CAP = 4


def code_block(key, full_shape):
    return jax.random.randint(key, full_shape, -127, 128).astype(jnp.float32).astype(jnp.bfloat16)


def draw_suffix_keys(key, part):
    return code_block(jax.random.fold_in(key, 11), (BEAMS, PAGES * PAGE, KV_HEADS * HEAD_DIM))


def draw_suffix_values(key, part):
    return code_block(jax.random.fold_in(key, 12), (BEAMS, PAGES * PAGE, KV_HEADS * HEAD_DIM))


def draw_prefix_keys(key, part):
    return code_block(jax.random.fold_in(key, 13), (PREFIX, KV_HEADS * HEAD_DIM))


def draw_prefix_values(key, part):
    return code_block(jax.random.fold_in(key, 14), (PREFIX, KV_HEADS * HEAD_DIM))


def draw_queries(key, part):
    base_key = jax.random.fold_in(key, 21)
    full_shape = (CHILDREN, HEADS * HEAD_DIM)
    values = jax.random.normal(base_key, full_shape, jnp.float32)
    return values.astype(jnp.bfloat16)


def draw_parents(key, part):
    groups = CHILDREN // CHILD_DEV
    pick_key = jax.random.fold_in(key, 31)
    order_key = jax.random.fold_in(key, 32)
    local_key = jax.random.fold_in(key, 33)
    favoured = jax.random.randint(pick_key, (), 0, groups).astype(jnp.int32)
    others = ((favoured + 1 + jnp.arange((groups - 1) * CAP, dtype=jnp.int32) // CAP) % groups).astype(jnp.int32)

    def one_block(block_key):
        perm_key = jax.random.fold_in(block_key, 1)
        mix_key = jax.random.fold_in(block_key, 2)
        chosen = jax.random.permutation(perm_key, others)[:CHILD_DEV - CAP]
        owners = jnp.concatenate([jnp.zeros((CAP,), jnp.int32) + favoured, chosen.astype(jnp.int32)])
        return jax.random.permutation(mix_key, owners)
    owners = jax.vmap(one_block)(jax.random.split(order_key, groups)).reshape(CHILDREN)
    local = jax.random.randint(local_key, (CHILDREN,), 0, BEAM_DEV).astype(jnp.int32)
    return (owners * BEAM_DEV + local).astype(jnp.int32)


def place_ends(entries, key, least, top_value):
    index_at = [jax.random.randint(jax.random.fold_in(key, axis), (), 0, length) for axis, length in enumerate(entries.shape)]
    longest = entries.shape.index(max(entries.shape))
    next_to = index_at[:longest] + [(index_at[longest] + 1) % entries.shape[longest]] + index_at[longest + 1:]
    return entries.at[tuple(index_at)].set(least).at[tuple(next_to)].set(top_value)


def levels(key, dims, cuts, least, top_value):
    gain, own = 1.0, jax.random.fold_in(key, 6)
    for position, shards_of in cuts:
        heights = jnp.exp(jax.random.uniform(jax.random.fold_in(own, position), (shards_of,), jnp.float32, least / len(cuts), top_value / len(cuts)))
        gain = gain * jnp.repeat(heights, dims[position] // shards_of).reshape([-1 if axis == position else 1 for axis in range(len(dims))])
    return gain


def normal_values(key, dims, deviation, limit, pieces=(), held_as=jnp.bfloat16):
    entries = jax.random.normal(key, dims, jnp.float32) * deviation
    if len(pieces) > 0:
        entries = levels(key, dims, pieces, -0.22, 0.18) * entries
    return jnp.clip(entries, min=-limit, max=limit).astype(held_as)


def setup_inputs(seed: int = 0, part: int = 0) -> dict:
    seeds = jax.random.split(jax.random.key(seed), 12)
    part_keys = jax.random.split(jax.random.fold_in(seeds[11], part), 12)
    queries = draw_queries(jax.random.fold_in(jax.random.fold_in(seeds[11], part), 71), part)
    new_keys = normal_values(part_keys[1], (CHILDREN, KV_HEADS * HEAD_DIM), 3.0, 18.0, ((0, 8),))
    new_values = normal_values(part_keys[2], (CHILDREN, KV_HEADS * HEAD_DIM), 2.0, 12.0, ((0, 8),))
    parents = draw_parents(jax.random.fold_in(jax.random.fold_in(seeds[11], part), 71), part)
    page_counts = place_ends(jax.random.randint(part_keys[4], (BEAMS,), 1, PAGES + 1), jax.random.fold_in(part_keys[4], 1), 1, PAGES).astype(jnp.int32)
    suffix_keys = draw_suffix_keys(jax.random.fold_in(jax.random.fold_in(seeds[11], part), 71), part)
    suffix_values = draw_suffix_values(jax.random.fold_in(jax.random.fold_in(seeds[11], part), 71), part)
    suffix_scales = jnp.clip(jnp.exp(math.log(0.044921875) - 0.58996294 * jax.random.uniform(part_keys[7], (BEAMS, PAGES, 2, KV_HEADS), jnp.float32) ** levels(part_keys[7], (BEAMS, PAGES, 2, KV_HEADS), ((0, 8),), -0.2, 0.2)), 0.024902344, 0.044921875).astype(jnp.bfloat16)
    prefix_keys = draw_prefix_keys(jax.random.fold_in(jax.random.fold_in(seeds[11], part), 71), part)
    prefix_values = draw_prefix_values(jax.random.fold_in(jax.random.fold_in(seeds[11], part), 71), part)
    prefix_scales = jnp.clip(jnp.exp(math.log(0.029907227) - 0.916290732 * jax.random.uniform(part_keys[10], (PREFIX // PAGE, 2, KV_HEADS), jnp.float32) ** levels(part_keys[10], (PREFIX // PAGE, 2, KV_HEADS), ((0, 8),), -0.2, 0.2)), 0.011962891, 0.029907227).astype(jnp.bfloat16)
    return {"queries": queries, "new_keys": new_keys, "new_values": new_values, "parents": parents, "page_counts": page_counts, "suffix_keys": suffix_keys, "suffix_values": suffix_values, "suffix_scales": suffix_scales, "prefix_keys": prefix_keys, "prefix_values": prefix_values, "prefix_scales": prefix_scales}


def page_parts(query_heads, key_codes, value_codes, scales):
    page_count = scales.shape[0]
    key_rows = key_codes.astype(jnp.float32).reshape(page_count, PAGE, KV_HEADS, HEAD_DIM)
    value_rows = value_codes.astype(jnp.float32).reshape(page_count, PAGE, KV_HEADS, HEAD_DIM)
    scale_rows = scales.astype(jnp.float32)
    scores = jnp.einsum("kgd,ptkd->pkgt", query_heads, key_rows)
    scores = scores * (scale_rows[:, 0, :] * HEAD_DIM ** -0.5)[:, :, None, None]
    maxima = jnp.max(scores, axis=-1)
    weights = jnp.exp(scores - maxima[..., None])
    totals = jnp.sum(weights, axis=-1)
    rounded = lax.optimization_barrier(weights.astype(jnp.bfloat16)).astype(jnp.float32)
    partial_value = jnp.einsum("pkgt,ptkd->pkgd", rounded, value_rows)
    partial_value = partial_value * scale_rows[:, 1, :][:, :, None, None]
    return maxima, totals, partial_value


def reference(queries, new_keys, new_values, parents, page_counts, suffix_keys, suffix_values, suffix_scales, prefix_keys, prefix_values, prefix_scales):
    group_size = HEADS // KV_HEADS
    prefix_pages = prefix_scales.shape[0]

    def one_child(child_item):
        one_query, own_key, own_value, parent = child_item
        query_heads = one_query.astype(jnp.float32).reshape(KV_HEADS, group_size, HEAD_DIM)
        pre_max, pre_total, pre_sum = page_parts(query_heads, prefix_keys, prefix_values, prefix_scales)
        suf_max, suf_total, suf_sum = page_parts(query_heads, suffix_keys[parent], suffix_values[parent], suffix_scales[parent])
        live_pages = jnp.arange(PAGES, dtype=jnp.int32) < page_counts[parent]
        valid = jnp.concatenate([jnp.ones((prefix_pages,), dtype=bool), live_pages])
        maxima = jnp.concatenate([pre_max, suf_max], axis=0)
        totals = jnp.concatenate([pre_total, suf_total], axis=0)
        partial_value = jnp.concatenate([pre_sum, suf_sum], axis=0)
        own_keys = own_key.astype(jnp.float32).reshape(KV_HEADS, 1, HEAD_DIM)
        own_score = jnp.sum(query_heads * own_keys, axis=-1) * HEAD_DIM ** -0.5
        masked = jnp.where(valid[:, None, None], maxima, jnp.float32(-1.0e30))
        peak = jnp.maximum(jnp.max(masked, axis=0), own_score)
        factor = jnp.where(valid[:, None, None], jnp.exp(masked - peak[None]), jnp.float32(0.0))
        own_factor = jnp.exp(own_score - peak)
        total = jnp.sum(factor * totals, axis=0) + own_factor
        own_values = own_value.astype(jnp.float32).reshape(KV_HEADS, 1, HEAD_DIM)
        summed = jnp.sum(factor[..., None] * partial_value, axis=0) + own_factor[..., None] * own_values
        return (summed / total[..., None]).reshape(HEADS * HEAD_DIM).astype(jnp.bfloat16)

    return lax.map(one_child, (queries, new_keys, new_values, parents))
```

```python
import functools
import math

import jax
import jax.numpy as jnp
from jax import lax
from jax.experimental import pallas as pl
from jax.experimental.pallas import tpu as pltpu
from jax.sharding import PartitionSpec as P

HEADS = 32
KV_HEADS = 8
HEAD_DIM = 128
GROUP = HEADS // KV_HEADS

NEG_FILL = -1e30
LOG2E = math.log2(math.e)
SCORE_FACTOR = HEAD_DIM ** (-0.5) * LOG2E


class Sizes:
    def __init__(self, groups, child_count, beam_count, page, page_count):
        self.groups = groups
        self.children = child_count
        self.beams = beam_count
        self.page = page
        self.pages = page_count
        self.slots = max(4, 2 * child_count // groups)
        self.tile = GROUP * self.slots
        self.at_query = 2 * page
        self.at_slot = self.at_query + GROUP * child_count
        self.at_scale = self.at_slot + KV_HEADS * self.tile
        self.at_which = self.at_scale + 16
        self.send_rows = self.at_which + self.tile
        self.at_prefix = KV_HEADS * self.tile
        self.at_stat = self.at_prefix + GROUP * child_count
        self.stat_rows = max(self.tile, child_count)
        self.back_rows = self.at_stat + self.stat_rows
        self.lane_total = KV_HEADS
        self.lane_pre = 2 * KV_HEADS
        self.lane_pre_total = self.lane_pre + HEADS


def lanes_of(head):
    start = head * HEAD_DIM
    if not isinstance(head, int):
        start = pl.multiple_of(start, HEAD_DIM)
    return pl.ds(start, HEAD_DIM)


def lane_index(shape):
    return lax.broadcasted_iota(jnp.int32, shape, len(shape) - 1)


def pack_kernel(sz, parents_ref, query_ref, key_ref, value_ref, scale_ref, *outs):
    outs, slot_ref = outs[:-1], outs[-1]
    me = lax.axis_index("beam")
    owners = [lax.div(parents_ref[c], sz.beams) for c in range(sz.children)]
    locals_ = [lax.rem(parents_ref[c], sz.beams) for c in range(sz.children)]
    width = GROUP * sz.children
    child_of = lax.rem(lane_index((1, width)), sz.children)
    slot_of = jnp.zeros((1, width), jnp.int32)
    local_of = jnp.zeros((1, width), jnp.int32)
    for c in range(sz.children):
        rank = jnp.int32(0)
        for other in range(c):
            rank = rank + (owners[other] == owners[c]).astype(jnp.int32)
        slot = (owners[c] ^ me) * sz.slots + rank
        slot_ref[c] = slot
        slot_of = jnp.where(child_of == c, slot, slot_of)
        local_of = jnp.where(child_of == c, locals_[c], local_of)

    rows = sz.groups * sz.tile
    row = lax.broadcasted_iota(jnp.int32, (rows, width), 0)
    column = lane_index((rows, width))
    row_slot = lax.div(row, sz.tile) * sz.slots + lax.rem(row, sz.slots)
    row_group = lax.rem(lax.div(row, sz.slots), GROUP)
    match = (row_slot == slot_of) & (row_group == lax.div(column, sz.children))
    dispatch = jnp.where(match, 1.0, 0.0).astype(jnp.bfloat16)
    which = jnp.where(match, local_of.astype(jnp.float32), 0.0).astype(jnp.bfloat16)
    which = jnp.dot(
        which, jnp.ones((width, HEAD_DIM), jnp.bfloat16), preferred_element_type=jnp.float32
    ).astype(jnp.bfloat16)
    scales = scale_ref[0].astype(jnp.float32)
    scale_lane = lane_index(scales.shape)
    scale_row = lax.broadcasted_iota(jnp.int32, (16, HEAD_DIM), 0)
    for k, out in enumerate(outs):
        head = lax.rem(me ^ k, KV_HEADS)
        out[0 : sz.page, :] = key_ref[:, lanes_of(head)]
        out[sz.page : 2 * sz.page, :] = value_ref[:, lanes_of(head)]
        for g in range(GROUP):
            start = sz.at_query + g * sz.children
            out[start : start + sz.children, :] = query_ref[:, lanes_of(head * GROUP + g)]
        own = jnp.sum(jnp.where(scale_lane == head, scales, 0.0), axis=1, keepdims=True)
        out[sz.at_scale : sz.at_scale + 16, :] = jnp.where(
            scale_row == 0, own[0:1, :], own[1:2, :]
        ).astype(jnp.bfloat16)
        out[sz.at_which : sz.at_which + sz.tile, :] = which[k * sz.tile : (k + 1) * sz.tile]
    for kv in range(KV_HEADS):
        stacked = jnp.concatenate(
            [query_ref[:, lanes_of(kv * GROUP + g)] for g in range(GROUP)], axis=0
        )
        moved = jnp.dot(dispatch, stacked, preferred_element_type=jnp.float32)
        moved = moved.astype(jnp.bfloat16)
        start = sz.at_slot + kv * sz.tile
        for k, out in enumerate(outs):
            out[start : start + sz.tile, :] = moved[k * sz.tile : (k + 1) * sz.tile]


def own_kernel(sz, query_ref, key_ref, out_ref):
    lane = lane_index((sz.children, HEAD_DIM))
    for g in range(GROUP):
        packed = jnp.zeros((sz.children, HEAD_DIM), jnp.float32)
        for kv in range(KV_HEADS):
            product = query_ref[:, lanes_of(kv * GROUP + g)].astype(jnp.float32) * key_ref[
                :, lanes_of(kv)
            ].astype(jnp.float32)
            score = jnp.sum(product, axis=1, keepdims=True) * SCORE_FACTOR
            packed = jnp.where(lane == kv, score, packed)
        out_ref[g * sz.children : (g + 1) * sz.children, :] = packed


def page_softmax(scores, page, key_scales):
    maxima, totals, weights = [], [], []
    for p, key_scale in enumerate(key_scales):
        scaled = scores[:, p * page : (p + 1) * page] * key_scale
        highest = jnp.max(scaled, axis=1, keepdims=True)
        weight = jnp.exp2(scaled - highest)
        maxima.append(highest)
        totals.append(jnp.sum(weight, axis=1, keepdims=True))
        weights.append(weight.astype(jnp.bfloat16))
    return maxima, totals, weights


def attend_kernel(sz, count_ref, scale_ref, *refs):
    bufs = refs[: sz.groups]
    keys_ref, values_ref = refs[sz.groups : sz.groups + 2]
    outs = refs[sz.groups + 2 : 2 * sz.groups + 2]
    me = lax.axis_index("beam")
    my_head = lax.rem(me, KV_HEADS)
    near = min(sz.groups, KV_HEADS)
    contract_last = (((1,), (1,)), ((), ()))

    def scale_at(beam, p, part, kv):
        return scale_ref[((beam * sz.pages + p) * 2 + part) * KV_HEADS + kv]

    rows = sz.groups * sz.tile
    which = jnp.concatenate(
        [b[sz.at_which : sz.at_which + sz.tile, :] for b in bufs], axis=0
    )
    which_f = which.astype(jnp.float32)
    picks_f = [jnp.where(which_f == b, 1.0, 0.0) for b in range(sz.beams)]
    picks = [x.astype(jnp.bfloat16) for x in picks_f]
    lane = lane_index((rows, HEAD_DIM))
    stats = jnp.zeros((rows, HEAD_DIM), jnp.float32)

    def by_beam(values):
        chosen = values[0]
        for b in range(1, sz.beams):
            chosen = jnp.where(which_f == b, values[b], chosen)
        return chosen

    for kv in range(KV_HEADS):
        start = sz.at_slot + kv * sz.tile
        query = jnp.concatenate([b[start : start + sz.tile, :] for b in bufs], axis=0)
        query = jnp.concatenate([query * x for x in picks], axis=1)
        key = jnp.concatenate([keys_ref[b, :, lanes_of(kv)] for b in range(sz.beams)], axis=1)
        scores = lax.dot_general(query, key, contract_last, preferred_element_type=jnp.float32)
        key_scales = [
            by_beam([scale_at(b, p, 0, kv) * SCORE_FACTOR for b in range(sz.beams)])
            for p in range(sz.pages)
        ]
        maxima, totals, weights = page_softmax(scores, sz.page, key_scales)
        highest = None
        for p in range(sz.pages):
            floor = by_beam(
                [jnp.where(p < count_ref[b], 0.0, NEG_FILL) for b in range(sz.beams)]
            )
            maxima[p] = jnp.where(floor < 0.0, NEG_FILL, maxima[p])
            highest = maxima[p] if p == 0 else jnp.maximum(highest, maxima[p])
        total, summed = None, None
        for p in range(sz.pages):
            factor = jnp.exp2(maxima[p] - highest)
            weight = jnp.concatenate([weights[p] * x for x in picks], axis=1)
            value = jnp.concatenate(
                [
                    values_ref[b, p * sz.page : (p + 1) * sz.page, lanes_of(kv)]
                    for b in range(sz.beams)
                ],
                axis=0,
            )
            part = jnp.dot(weight, value, preferred_element_type=jnp.float32)
            value_scale = by_beam([scale_at(b, p, 1, kv) for b in range(sz.beams)])
            part = part * (factor * value_scale)
            total = factor * totals[p] if p == 0 else total + factor * totals[p]
            summed = part if p == 0 else summed + part
        stats = jnp.where(lane == kv, highest, stats)
        stats = jnp.where(lane == sz.lane_total + kv, total, stats)
        for k, out in enumerate(outs):
            out[kv * sz.tile : (kv + 1) * sz.tile, :] = summed[k * sz.tile : (k + 1) * sz.tile]

    key = jnp.concatenate([b[0 : sz.page, :] for b in bufs], axis=0)
    key_scales, value_scales = [], []
    for b in bufs:
        pair = b[sz.at_scale : sz.at_scale + 16, :].astype(jnp.float32)
        key_scales.append(pair[0:1, :] * SCORE_FACTOR)
        value_scales.append(pair[1:2, :])
    lane = lane_index((sz.children, HEAD_DIM))
    for k in range(sz.groups):
        stat = stats[k * sz.tile : (k + 1) * sz.tile]
        if k < near:
            query = bufs[k][sz.at_query : sz.at_query + GROUP * sz.children, :]
            scores = lax.dot_general(
                query, key, contract_last, preferred_element_type=jnp.float32
            )
            maxima, totals, weights = page_softmax(scores, sz.page, key_scales)
            highest = functools.reduce(jnp.maximum, maxima)
            total, summed = None, None
            for p, b in enumerate(bufs):
                factor = jnp.exp2(maxima[p] - highest)
                part = jnp.dot(
                    weights[p],
                    b[sz.page : 2 * sz.page, :],
                    preferred_element_type=jnp.float32,
                )
                part = part * (factor * value_scales[p])
                total = factor * totals[p] if p == 0 else total + factor * totals[p]
                summed = part if p == 0 else summed + part
            outs[k][sz.at_prefix : sz.at_prefix + GROUP * sz.children, :] = summed
            for g in range(GROUP):
                at = slice(g * sz.children, (g + 1) * sz.children)
                place = sz.lane_pre + g * KV_HEADS + my_head
                stat = jnp.where(lane == place, highest[at], stat)
                place = sz.lane_pre_total + g * KV_HEADS + my_head
                stat = jnp.where(lane == place, total[at], stat)
        else:
            empty = jnp.zeros((GROUP * sz.children, HEAD_DIM), jnp.float32)
            outs[k][sz.at_prefix : sz.at_prefix + GROUP * sz.children, :] = empty
        outs[k][sz.at_stat : sz.at_stat + sz.stat_rows, :] = stat


def join_kernel(sz, slot_ref, own_ref, value_ref, *refs):
    backs = refs[: sz.groups]
    out_ref, all_ref, sums_ref, stats_ref = refs[sz.groups :]
    me = lax.axis_index("beam")
    my_head = lax.rem(me, KV_HEADS)
    near = min(sz.groups, KV_HEADS)
    for k, back in enumerate(backs):
        all_ref[k * sz.back_rows : (k + 1) * sz.back_rows, :] = back[...]
    for c in range(sz.children):
        slot = slot_ref[c]
        start = lax.div(slot, sz.slots) * sz.back_rows + lax.rem(slot, sz.slots)
        sums_ref[pl.ds(c, HEADS, stride=sz.children), :] = all_ref[
            pl.ds(start, HEADS, stride=sz.slots), :
        ]
        stats_ref[pl.ds(c, GROUP, stride=sz.children), :] = all_ref[
            pl.ds(start + sz.at_stat, GROUP, stride=sz.slots), :
        ]
    pre = backs[0][sz.at_stat : sz.at_stat + sz.children, :]
    for k in range(1, near):
        pre = pre + backs[k][sz.at_stat : sz.at_stat + sz.children, :]

    def shifted(x, lanes):
        return pltpu.roll(x, HEAD_DIM - lanes, 1)

    coefficients = []
    for g in range(GROUP):
        at = slice(g * sz.children, (g + 1) * sz.children)
        suffix = stats_ref[at, :]
        suffix_total = shifted(suffix, sz.lane_total)
        prefix = shifted(pre, sz.lane_pre + g * KV_HEADS)
        prefix_total = shifted(pre, sz.lane_pre_total + g * KV_HEADS)
        own = own_ref[at, :]
        peak = jnp.maximum(jnp.maximum(prefix, suffix), own)
        suffix, prefix, own = (jnp.exp2(x - peak) for x in (suffix, prefix, own))
        total = prefix * prefix_total + suffix * suffix_total + own
        coefficients.append([x / total for x in (prefix, suffix, own)])

    shape = (sz.children, HEAD_DIM)
    for kv in range(KV_HEADS):
        source = (my_head ^ kv) * sz.back_rows + sz.at_prefix
        new_value = value_ref[:, lanes_of(kv)].astype(jnp.float32)
        for g in range(GROUP):
            prefix, suffix, own = (
                jnp.broadcast_to(x[:, kv : kv + 1], shape) for x in coefficients[g]
            )
            at = pl.multiple_of(source + g * sz.children, 8)
            head = kv * GROUP + g
            result = (
                prefix * all_ref[pl.ds(at, sz.children), :]
                + suffix * sums_ref[head * sz.children : (head + 1) * sz.children, :]
                + own * new_value
            )
            out_ref[:, lanes_of(head)] = result.astype(out_ref.dtype)


def whole(count, space=pltpu.VMEM):
    return [pl.BlockSpec(memory_space=space)] * count


def exchanged(pieces):
    groups = len(pieces)
    moved = list(pieces)
    order = sorted(range(1, groups), key=lambda k: (-(k // 2), k))
    for k in order:
        moved[k] = lax.ppermute(pieces[k], "beam", [(i, i ^ k) for i in range(groups)])
    return moved


def local(
    queries,
    new_keys,
    new_values,
    parents,
    page_counts,
    suffix_keys,
    suffix_values,
    suffix_scales,
    prefix_keys,
    prefix_values,
    prefix_scales,
):
    groups = lax.axis_size("beam")
    sz = Sizes(
        groups,
        queries.shape[0],
        suffix_keys.shape[0],
        prefix_keys.shape[0] // prefix_scales.shape[0],
        suffix_scales.shape[1],
    )
    send = jax.ShapeDtypeStruct((sz.send_rows, HEAD_DIM), jnp.bfloat16)
    back = jax.ShapeDtypeStruct((sz.back_rows, HEAD_DIM), jnp.float32)
    smem = pltpu.SMEM
    *pieces, slots = pl.pallas_call(
        functools.partial(pack_kernel, sz),
        out_shape=[send] * groups + [jax.ShapeDtypeStruct((sz.children,), jnp.int32)],
        in_specs=whole(1, smem) + whole(4),
        out_specs=whole(groups) + whole(1, smem),
        name="pack",
    )(parents, queries, prefix_keys, prefix_values, prefix_scales)
    own = pl.pallas_call(
        functools.partial(own_kernel, sz),
        out_shape=jax.ShapeDtypeStruct((GROUP * sz.children, HEAD_DIM), jnp.float32),
        in_specs=whole(2),
        out_specs=whole(1)[0],
        name="own",
    )(queries, new_keys)
    pieces = exchanged(pieces)
    backs = pl.pallas_call(
        functools.partial(attend_kernel, sz),
        out_shape=[back] * groups,
        in_specs=whole(2, smem) + whole(groups + 2),
        out_specs=whole(groups),
        name="attend",
    )(
        page_counts,
        suffix_scales.astype(jnp.float32).reshape(-1),
        *pieces,
        suffix_keys,
        suffix_values,
    )
    backs = exchanged(backs)
    rows = GROUP * sz.children
    return pl.pallas_call(
        functools.partial(join_kernel, sz),
        out_shape=jax.ShapeDtypeStruct(queries.shape, jnp.bfloat16),
        in_specs=whole(1, smem) + whole(groups + 2),
        out_specs=whole(1)[0],
        scratch_shapes=[
            pltpu.VMEM((groups * sz.back_rows, HEAD_DIM), jnp.float32),
            pltpu.VMEM((HEADS * sz.children, HEAD_DIM), jnp.float32),
            pltpu.VMEM((rows, HEAD_DIM), jnp.float32),
        ],
        name="join",
    )(slots, own, new_values, *backs)


def solution(mesh):
    in_specs = (
        P(("prob", "beam"), None),
        P(("prob", "beam"), None),
        P(("prob", "beam"), None),
        P(("prob", "beam")),
        P(("prob", "beam")),
        P(("prob", "beam"), None, None),
        P(("prob", "beam"), None, None),
        P(("prob", "beam"), None, None, None),
        P(("prob", "beam"), None),
        P(("prob", "beam"), None),
        P(("prob", "beam"), None, None),
    )
    out_specs = P(("prob", "beam"), None)
    return jax.shard_map(local, mesh=mesh, in_specs=in_specs, out_specs=out_specs, check_vma=False)
```
